32 devices in a mesh: rep: 4 (over z), inst: 8 (over y, x, core).
Axes of the slice: x: 2, y: 2, z: 4, core: 2. Of those that a mesh axis runs over, the one named last changes fastest.
Arguments:
- acts: bfloat16 [32768, 4096], P(('rep', 'inst')), may hold values from -6 to 6
- grad_keys: bfloat16 [32768, 1024], P(('rep', 'inst')), may hold values from -0.0625 to 0.0625
- grad_values: bfloat16 [32768, 1024], P(('rep', 'inst')), may hold values from -0.0625 to 0.0625
- grad_logits: bfloat16 [8, 32768], P(None, ('rep', 'inst')), may hold values from -0.0625 to 0.0625
- order: int32 [32], replicated, may hold values from 0 to 31, each once
- bucket_param: float32 [4, 2048, 1024], P(None, 'inst'), may hold values from -6 to 6
- bucket_m: float32 [4, 2048, 1024], P(None, 'inst'), may hold values from -6 to 6
- bucket_v: float32 [4, 2048, 1024], P(None, 'inst'), may hold values from 0.25 to 4
- router_param: float32 [32, 1024], P('inst'), may hold values from -6 to 6
- router_m: float32 [32, 1024], P('inst'), may hold values from -6 to 6
- router_v: float32 [32, 1024], P('inst'), may hold values from 0.25 to 4
Outputs:
- new_param: float32 [4, 2048, 1024], P(None, 'inst')
- new_moment: float32 [4, 2048, 1024], P(None, 'inst')
- new_second: float32 [4, 2048, 1024], P(None, 'inst')
- router_new_param: float32 [32, 1024], P('inst')
- router_new_moment: float32 [32, 1024], P('inst')
- router_new_second: float32 [32, 1024], P('inst')
The draws below stay inside these ranges and needn't reach their ends.
Inputs may be any that keep to these rules, and one draw needn't show every extreme that they name: order is a permutation of the 32 row blocks; entries with k * 8 <= s < (k + 1) * 8 fill bucket k.
All inputs are finite; a program needn't handle non-finite values.
Results may differ from the reference program's by a relative error of at most 0.0003.
Values sent between devices are 32-bit elements; how exact they have to be, the bound alone decides.
A program may use at most 256 MiB of HBM per device.

```python
import math
import jax
import jax.numpy as jnp
from jax import lax

D = 4096
KV = 1024
EXPERTS = 8
BUCKETS = 4
BLOCK_ROWS = 256
TOKENS = 32768
BLOCKS = 32
BUCKET_ROWS = 2048
ROUTER_ROWS = 32


def levels(rng, extent, split, least, high):
    factor_of, own = 1.0, jax.random.fold_in(rng, 6)
    for axis_at, parts in split:
        steps = jnp.exp(jax.random.uniform(jax.random.fold_in(own, axis_at), (parts,), jnp.float32, least / len(split), high / len(split)))
        factor_of = factor_of * jnp.repeat(steps, extent[axis_at] // parts).reshape([-1 if axis == axis_at else 1 for axis in range(len(extent))])
    return factor_of


def centred(own_key, dims, spread, most, shards=(), dtype=jnp.bfloat16):
    entries = spread * jax.random.normal(own_key, dims, jnp.float32)
    if shards:
        entries = entries * levels(own_key, dims, shards, -0.22, 0.18)
    return jnp.clip(entries, -most, most).astype(dtype)


def setup_inputs(seed: int = 0) -> dict:
    arg_keys = jax.random.split(jax.random.key(seed), 12)
    acts = centred(arg_keys[0], (TOKENS, D), 1.0, 6.0, ((0, 32),))
    grad_keys = centred(arg_keys[1], (TOKENS, KV), (TOKENS // 4) ** -0.5, 0.0625, ((0, 32),))
    grad_values = centred(arg_keys[2], (TOKENS, KV), (TOKENS // 4) ** -0.5, 0.0625, ((0, 32),))
    grad_logits = centred(arg_keys[3], (EXPERTS, TOKENS), (TOKENS // 4) ** -0.5, 0.0625, ((1, 32),))
    order = jax.random.permutation(arg_keys[4], BLOCKS).astype(jnp.int32)
    bucket_param = centred(arg_keys[5], (BUCKETS, BUCKET_ROWS, KV), 1.0, 6.0, ((1, 8),), jnp.float32)
    bucket_m = centred(arg_keys[6], (BUCKETS, BUCKET_ROWS, KV), 1.0, 6.0, ((1, 8),), jnp.float32)
    bucket_v = jnp.clip(jnp.exp(math.log(4.0) - 2.7725887 * jax.random.uniform(arg_keys[7], (BUCKETS, BUCKET_ROWS, KV), jnp.float32) ** levels(arg_keys[7], (BUCKETS, BUCKET_ROWS, KV), ((1, 8),), -0.2, 0.2)), 0.25, 4.0)
    router_param = centred(arg_keys[8], (ROUTER_ROWS, KV), 1.0, 6.0, ((0, 8),), jnp.float32)
    router_m = centred(arg_keys[9], (ROUTER_ROWS, KV), 1.0, 6.0, ((0, 8),), jnp.float32)
    router_v = jnp.clip(jnp.exp(math.log(4.0) - 2.7725887 * jax.random.uniform(arg_keys[10], (ROUTER_ROWS, KV), jnp.float32) ** levels(arg_keys[10], (ROUTER_ROWS, KV), ((0, 8),), -0.2, 0.2)), 0.25, 4.0)
    return {"acts": acts, "grad_keys": grad_keys, "grad_values": grad_values, "grad_logits": grad_logits, "order": order, "bucket_param": bucket_param, "bucket_m": bucket_m, "bucket_v": bucket_v, "router_param": router_param, "router_m": router_m, "router_v": router_v}


beta_first = 0.9
beta_second = 0.95
step_rate = 0.05
decay_rate = 0.1
epsilon = 1e-08
correct_first = 1.0 - 0.9 ** 10
correct_second = 1.0 - 0.95 ** 10

def contract(left, right):
    return lax.dot_general(left, right, (((0,), (0,)), ((), ())), preferred_element_type=jnp.float32)

def adamw(grad, param, moment, second):
    moment_new = beta_first * moment + (1.0 - beta_first) * grad
    second_new = beta_second * second + (1.0 - beta_second) * grad * grad
    ratio = moment_new / correct_first / (jnp.sqrt(second_new / correct_second) + epsilon)
    param_new = param - step_rate * (ratio + decay_rate * param)
    return (param_new, moment_new, second_new)

def reference(acts, grad_keys, grad_values, grad_logits, order, bucket_param, bucket_m, bucket_v, router_param, router_m, router_v):
    weight_rows = jnp.concatenate([contract(acts, grad_keys), contract(acts, grad_values)], axis=0)
    blocks = weight_rows.reshape(BLOCKS, BLOCK_ROWS, KV)
    packed = jnp.take(blocks, order.astype(jnp.int32), axis=0).reshape(BUCKETS, BUCKET_ROWS, KV)
    router_grad = jnp.dot(grad_logits, acts, preferred_element_type=jnp.float32).reshape(ROUTER_ROWS, KV)
    new_param, new_moment, new_second = adamw(packed, bucket_param, bucket_m, bucket_v)
    router_new_param, router_new_moment, router_new_second = adamw(router_grad, router_param, router_m, router_v)
    return (new_param, new_moment, new_second, router_new_param, router_new_moment, router_new_second)
```

```python
import functools

import jax
import jax.numpy as jnp
from jax import lax
from jax.experimental import pallas as pl
from jax.experimental.pallas import tpu as pltpu
from jax.sharding import PartitionSpec as P

MESH = pl.DeviceIdType.MESH
BUCKETS = 4
BLOCK_ROWS = 256
COLS = 128
SPLIT = 4
LAG = 4
HOP = 4
NEAR = 16
FAR = 32
FRONT = 10
FRONT_TWO = 0
ROUTER_START = 10
VMEM_BYTES = 36 * 2**20


beta_first = 0.9
beta_second = 0.95
step_rate = 0.05
decay_rate = 0.1
epsilon = 1e-08
correct_first = 1.0 - 0.9**10
correct_second = 1.0 - 0.95**10


def adamw(grad, param, moment, second):
    moment_new = beta_first * moment + (1.0 - beta_first) * grad
    second_new = beta_second * second + (1.0 - beta_second) * grad * grad
    ratio = moment_new / correct_first / (jnp.sqrt(second_new / correct_second) + epsilon)
    param_new = param - step_rate * (ratio + decay_rate * param)
    return (param_new, moment_new, second_new)


def both(*terms):
    return functools.reduce(jnp.logical_and, terms)


def whole_part(p):
    return lax.div(p, SPLIT), lax.rem(p, SPLIT)


def is_mixed(chunk, turn):
    last = both(turn == SPLIT - 1, jnp.logical_or(chunk < FRONT, lax.rem(chunk, 2) == 0))
    if FRONT_TWO:
        last = jnp.logical_or(last, both(turn == SPLIT - 2, chunk < FRONT_TWO))
    return last


MIXED_TURNS = (SPLIT - 2, SPLIT - 1) if FRONT_TWO else (SPLIT - 1,)


class Place:
    def __init__(self, n_inst, n_rep):
        self.n_inst, self.n_rep = n_inst, n_rep
        self.bits = n_inst.bit_length() - 1
        self.me, self.rep = lax.axis_index("inst"), lax.axis_index("rep")
        self.left = n_rep // 2 - 1
        low = self.rep <= self.left
        self.depth = jnp.where(low, self.rep, n_rep - 1 - self.rep)
        way = jnp.where(low, 1, -1)
        self.inner, self.outer = self.rep + way, self.rep - way
        self.flips = [(1 - 2 * ((self.me // 2**bit) % 2)) * 2**bit for bit in range(self.bits)]
        self.mixes = n_rep >= 4
        self.mate = jnp.where(self.depth == 0, self.inner, self.outer)
        self.edge = self.depth <= 1
        self.base = 1 + LAG * (self.bits - 1)
        self.top = self.base + HOP * (self.left + 1)
        self.last_step = self.top + HOP * self.left


class Lane:
    def __init__(self, place, kind, dims, refs, sems, finish):
        self.place, self.kind, self.dims = place, kind, dims
        self.parts, self.halves, self.outs, self.ins, self.raws = refs
        self.send, self.recv, self.raw_send, self.raw_recv = sems
        self.finish = finish
        self.stages = len(dims)

    def owner(self, q):
        index = self.place.me
        for at, bit in enumerate(self.dims):
            flip = lax.rem(lax.div(q, 2 ** (self.stages - 1 - at)), 2)
            index = index + flip * self.place.flips[bit]
        return index

    def half_copy(self, stage, p):
        count = self.place.n_inst >> (stage + 1)
        source = self.parts(p) if stage == 0 else self.halves(stage - 1, p)
        return pltpu.make_async_remote_copy(
            src_ref=source.at[pl.ds(count, count)],
            dst_ref=self.halves(stage, p),
            send_sem=self.send.at[stage, p],
            recv_sem=self.recv.at[stage, p],
            device_id={"inst": self.place.me + self.place.flips[self.dims[stage]]},
            device_id_type=MESH,
        )

    def arrive(self, stage, p):
        self.half_copy(stage, p).wait()
        count = self.place.n_inst >> (stage + 1)
        source = self.parts(p) if stage == 0 else self.halves(stage - 1, p)
        into = self.halves(stage, p)
        into[...] += source[pl.ds(0, count)]

    def raw_copy(self, p, at):
        return pltpu.make_async_remote_copy(
            src_ref=self.halves(0, p),
            dst_ref=self.raws(at),
            send_sem=self.raw_send.at[at],
            recv_sem=self.raw_recv.at[at],
            device_id={"rep": self.place.mate},
            device_id_type=MESH,
        )

    def total(self, p):
        return self.halves(self.stages - 1, p)

    def inward(self, p, middle):
        return pltpu.make_async_remote_copy(
            src_ref=self.total(p),
            dst_ref=self.ins(p) if middle else self.outs(p),
            send_sem=self.send.at[self.stages, p],
            recv_sem=self.recv.at[self.stages + 1 if middle else self.stages, p],
            device_id={"rep": self.place.inner},
            device_id_type=MESH,
        )

    def outward(self, p):
        return pltpu.make_async_remote_copy(
            src_ref=self.ins(p),
            dst_ref=self.ins(p),
            send_sem=self.send.at[self.stages + 1, p],
            recv_sem=self.recv.at[self.stages + 1, p],
            device_id={"rep": self.place.outer},
            device_id_type=MESH,
        )


def advance(place, lanes, t, count, mixes):
    mixes = mixes and place.mixes

    def due(lag, body):
        p = t - lag

        @pl.when(both(p >= 0, p < count))
        def _():
            body(p)

    def odd(lane, chunk, turn):
        return lax.rem(chunk + turn + lane.kind + place.depth, 2) == 1

    def each_lane(body):
        for lane in lanes:
            body(lane)

    def raw_at(chunk, turn):
        return chunk if turn == SPLIT - 1 else count // SPLIT + chunk

    def mixed(p, body):
        chunk, turn = whole_part(p)
        for fixed in MIXED_TURNS:

            @pl.when(both(turn == fixed, is_mixed(chunk, fixed)))
            def _():
                for lane in lanes:
                    takes = odd(lane, chunk, fixed)
                    body(lane, chunk, fixed, takes)

    def early(p, body):
        chunk, turn = whole_part(p)

        @pl.when(turn == 0)
        def _():
            for fixed in MIXED_TURNS:

                @pl.when(is_mixed(chunk, fixed))
                def _():
                    for lane in lanes:
                        body(lane, p + fixed, chunk, fixed)

    def plain(p, body):
        if not mixes:
            each_lane(body)
            return
        chunk, turn = whole_part(p)

        @pl.when(jnp.logical_not(is_mixed(chunk, turn)))
        def _():
            each_lane(body)

    def start(p):
        plain(p, lambda lane: lane.half_copy(0, p).start())
        if mixes:
            early(p, lambda lane, at, chunk, turn: lane.half_copy(0, at).start())

    due(0, start)

    def onward(lane, p):
        if place.bits > 1:
            lane.half_copy(1, p).start()

    def first(p):
        def usual(lane):
            lane.arrive(0, p)
            onward(lane, p)

        plain(p, usual)
        if not mixes:
            return

        def taken(lane, chunk, turn, takes):
            at = raw_at(chunk, turn)

            @pl.when(both(place.edge, takes))
            def _():
                lane.raw_copy(p, at).wait_recv()
                into = lane.halves(0, p)
                into[...] += lane.raws(at)[...]

            @pl.when(jnp.logical_or(jnp.logical_not(place.edge), takes))
            def _():
                onward(lane, p)

        mixed(p, taken)

        def given(lane, p, chunk, turn):
            lane.arrive(0, p)

            @pl.when(both(place.edge, jnp.logical_not(odd(lane, chunk, turn))))
            def _():
                lane.raw_copy(p, raw_at(chunk, turn)).start()

        early(p, given)

    due(1, first)

    def later(stage):
        def usual(lane, p):
            lane.arrive(stage, p)
            if stage < place.bits - 1:
                lane.half_copy(stage + 1, p).start()
            else:

                @pl.when(place.depth == 0)
                def _():
                    lane.inward(p, place.left == 0).start()

        def body(p):
            plain(p, lambda lane: usual(lane, p))
            if not mixes:
                return

            def special(lane, chunk, turn, takes):
                gives = both(place.edge, jnp.logical_not(takes))

                @pl.when(jnp.logical_not(gives))
                def _():
                    usual(lane, p)

                if stage == 1:

                    @pl.when(gives)
                    def _():
                        lane.raw_copy(p, raw_at(chunk, turn)).wait_send()

            mixed(p, special)

        return body

    for stage in range(1, place.bits):
        due(1 + LAG * stage, later(stage))

    def collect(p):
        def go(lane):
            if place.left == 1:
                lane.inward(p, True).start()
            else:
                for middle in (False, True):

                    @pl.when((place.depth == place.left) == middle)
                    def _():
                        lane.inward(p, middle).start()

        def usual(lane):
            lane.inward(p, False).wait_recv()
            into = lane.total(p)
            into[...] += lane.outs(p)[...]
            go(lane)

        def special(lane, chunk, turn, takes):
            near = place.depth == 1

            @pl.when(both(near, jnp.logical_not(takes)))
            def _():
                lane.inward(p, False).wait_recv()
                lane.total(p)[...] = lane.outs(p)[...]

            @pl.when(jnp.logical_not(near))
            def _():
                lane.inward(p, False).wait_recv()
                into = lane.total(p)
                into[...] += lane.outs(p)[...]

            go(lane)

        @pl.when(place.depth > 0)
        def _():
            plain(p, usual)
            if mixes:
                mixed(p, special)

    if place.left > 0:
        due(place.base + HOP * place.depth, collect)

    def share(p):
        for lane in lanes:
            lane.outward(p).wait_recv()

            @pl.when(place.depth == place.left)
            def _(lane=lane):
                into = lane.ins(p)
                into[...] += lane.total(p)[...]

            @pl.when(place.depth > 0)
            def _(lane=lane):
                lane.outward(p).start()

        for lane in lanes:
            lane.finish(p)

    due(place.top + HOP * (place.left - place.depth), share)

    def settle(p):
        def sent(lane):
            lane.inward(p, False).wait_send()

        plain(p, sent)
        if mixes:

            def special(lane, chunk, turn, takes):
                @pl.when(jnp.logical_or(place.depth > 0, takes))
                def _():
                    sent(lane)

            mixed(p, special)

        @pl.when(place.depth > 0)
        def _():
            for lane in lanes:
                lane.outward(p).wait_send()

    due(place.last_step, settle)


def kernel(n_inst, n_rep, *refs):
    order_in, acts, keys_in, values_in, logits_in = refs[:5]
    state_in, state = refs[5:11], refs[11:17]
    order, slabs, keys, values, logits, turned, router_all, parts, router_parts = refs[17:26]
    raws, load = refs[26:28]
    scratch = refs[28:]
    place = Place(n_inst, n_rep)
    bits, rep = place.bits, place.rep
    rows = slabs.shape[-1]
    width = router_parts.shape[-1]
    per_bucket = order.shape[0] // BUCKETS
    column_blocks = acts.shape[1] // BLOCK_ROWS
    chunks = keys.shape[1] // COLS
    every = chunks * BUCKETS // 2
    count = every * SPLIT
    size = COLS // SPLIT
    halves = scratch[:bits]
    router_halves = scratch[bits : 2 * bits]
    outs, ins, router_outs, router_ins = scratch[2 * bits : 2 * bits + 4]
    sends, recvs, router_sends, router_recvs, raw_sends, raw_recvs = scratch[2 * bits + 4 :]

    def finish(kind):
        def body(p):
            chunk, turn = whole_part(p)

            @pl.when(turn == SPLIT - 1)
            def _():
                bucket = 2 * lax.div(chunk, chunks) + kind
                start = pl.multiple_of(lax.rem(chunk, chunks) * COLS, COLS)
                slot = lax.rem(chunk * SPLIT, ins.shape[1])
                grad = ins[kind, pl.ds(slot, SPLIT), 0].reshape(COLS, rows).T
                at = (bucket, slice(None), pl.ds(start, COLS))
                fresh = adamw(grad, *[part[at] for part in state[:3]])
                for part, value in zip(state[:3], fresh):
                    part[at] = value

        return body

    def router_finish(p):
        line = state[3].shape[1]
        for at in range(state[3].shape[0]):
            one = (pl.ds(at, 1), slice(None))
            grad = router_ins[0, :, pl.ds(at * line, line)]
            fresh = adamw(grad, *[part[one] for part in state[3:]])
            for part, value in zip(state[3:], fresh):
                part[one] = value

    forward = [0] + list(range(1, bits))
    backward = [0] + list(range(bits - 1, 0, -1))
    lanes = []
    for kind, dims in enumerate((forward, backward)):
        lanes.append(
            Lane(
                place,
                kind,
                dims,
                (
                    lambda p, kind=kind: parts.at[kind, lax.rem(p, 2 * SPLIT)],
                    lambda stage, p, kind=kind: halves[stage].at[
                        kind, lax.rem(p, halves[stage].shape[1])
                    ],
                    lambda p, kind=kind: outs.at[kind, lax.rem(p, outs.shape[1])],
                    lambda p, kind=kind: ins.at[kind, lax.rem(p, ins.shape[1])],
                    lambda at: raws.at[at],
                ),
                (sends.at[kind], recvs.at[kind], raw_sends, raw_recvs),
                finish(kind),
            )
        )
    router = Lane(
        place,
        0,
        forward,
        (
            lambda p: router_parts,
            lambda stage, p: router_halves[stage],
            lambda p: router_outs,
            lambda p: router_ins,
            None,
        ),
        (router_sends, router_recvs, None, None),
        router_finish,
    )

    loads = [
        pltpu.make_async_copy(src, dst, load.at[at])
        for at, (src, dst) in enumerate(
            ((order_in, order), (keys_in, keys), (values_in, values), (logits_in, logits))
        )
    ]
    loads += [
        pltpu.make_async_copy(acts.at[:, pl.ds(at * rows, rows)], slabs.at[at], load.at[4 + at])
        for at in range(slabs.shape[0])
    ]
    states = [
        pltpu.make_async_copy(src, dst, load.at[4 + slabs.shape[0] + at])
        for at, (src, dst) in enumerate(zip(state_in, state))
    ]
    for copy in loads:
        copy.start()

    barrier = pltpu.get_barrier_semaphore()
    for flip in place.flips:
        pl.semaphore_signal(
            barrier, inc=1, device_id={"inst": place.me + flip}, device_id_type=MESH
        )

    @pl.when(rep > 0)
    def _():
        pl.semaphore_signal(barrier, inc=1, device_id={"rep": rep - 1}, device_id_type=MESH)

    @pl.when(rep < n_rep - 1)
    def _():
        pl.semaphore_signal(barrier, inc=1, device_id={"rep": rep + 1}, device_id_type=MESH)

    for copy in loads:
        copy.wait()
    for copy in states:
        copy.start()

    each = n_inst // SPLIT

    def products(chunk, turn):
        column = pl.multiple_of(lax.rem(chunk, chunks) * COLS, COLS)

        @pl.when(turn == 0)
        def _():
            turned[0] = keys[:, pl.ds(column, COLS)].T
            turned[1] = values[:, pl.ds(column, COLS)].T

        slot = lax.rem(chunk, 2) * SPLIT
        for kind, lane in enumerate(lanes):
            bucket = 2 * lax.div(chunk, chunks) + kind
            for i in range(each):
                q = turn * each + i
                first = lane.owner(q) * rows
                block = order[bucket * per_bucket + lax.div(first, BLOCK_ROWS)]
                at = lax.rem(block, column_blocks) * (BLOCK_ROWS // rows)
                at = at + lax.div(lax.rem(first, BLOCK_ROWS), rows)
                full = jnp.dot(
                    turned[lax.div(block, column_blocks)],
                    slabs[at],
                    preferred_element_type=jnp.float32,
                )
                for part in range(SPLIT):
                    parts[kind, slot + part, q] = full[part * size : (part + 1) * size]

    def router_products():
        for at in range(slabs.shape[0]):
            router_all[:, pl.ds(at * rows, rows)] = jnp.dot(
                logits[...], slabs[at], preferred_element_type=jnp.float32
            )
        for q in range(n_inst):
            first = router.owner(q) * width
            router_parts[q] = router_all[
                pl.ds(first // acts.shape[1], 1),
                pl.ds(pl.multiple_of(first % acts.shape[1], width), width),
            ]

    def head(turn, carry):
        products(0, turn)
        return carry

    lax.fori_loop(0, SPLIT, head, 0)
    peers = bits + jnp.where(rep > 0, 1, 0) + jnp.where(rep < n_rep - 1, 1, 0)
    pl.semaphore_wait(barrier, peers)

    def step(t, carry):
        advance(place, lanes, t, count, True)

        @pl.when(t == ROUTER_START)
        def _():
            router_products()
            for copy in states:
                copy.wait()

        @pl.when(both(t >= ROUTER_START, t <= ROUTER_START + place.last_step))
        def _():
            advance(place, [router], t - ROUTER_START, 1, False)

        @pl.when(t < count - SPLIT)
        def _():
            products(lax.div(t, SPLIT) + 1, lax.rem(t, SPLIT))

        return carry

    lax.fori_loop(0, count + place.last_step, step, 0)


def summed(order, acts, keys, values, logits, states, n_inst, n_rep):
    bits = n_inst.bit_length() - 1
    rows = states[0].shape[1]
    width = states[3].size
    kv = keys.shape[1]
    size = COLS // SPLIT
    every = kv // COLS * BUCKETS // 2
    count = every * SPLIT
    vmem = pl.BlockSpec(memory_space=pltpu.VMEM)
    f32 = jnp.float32
    scratch = [
        pltpu.SMEM(order.shape, order.dtype),
        pltpu.VMEM((acts.shape[1] // rows, acts.shape[0], rows), acts.dtype),
        pltpu.VMEM(keys.shape, keys.dtype),
        pltpu.VMEM(values.shape, values.dtype),
        pltpu.VMEM(logits.shape, logits.dtype),
        pltpu.VMEM((2, COLS, acts.shape[0]), acts.dtype),
        pltpu.VMEM((logits.shape[0], acts.shape[1]), f32),
        pltpu.VMEM((2, 2 * SPLIT, n_inst, size, rows), f32),
        pltpu.VMEM((n_inst, 1, width), f32),
        pltpu.VMEM((every + FRONT_TWO, n_inst // 2, size, rows), f32),
        pltpu.SemaphoreType.DMA((acts.shape[1] // rows + 4 + len(states),)),
    ]
    scratch += [
        pltpu.VMEM((2, min(count, FAR if s else NEAR), n_inst >> (s + 1), size, rows), f32)
        for s in range(bits)
    ]
    scratch += [pltpu.VMEM((n_inst >> (s + 1), 1, width), f32) for s in range(bits)]
    scratch += [pltpu.VMEM((2, min(count, FAR), 1, size, rows), f32)] * 2
    scratch += [pltpu.VMEM((1, 1, width), f32)] * 2
    scratch += [pltpu.SemaphoreType.DMA((2, bits + 2, count))] * 2
    scratch += [pltpu.SemaphoreType.DMA((bits + 2, 1))] * 2
    scratch += [pltpu.SemaphoreType.DMA((every + FRONT_TWO,))] * 2
    operands = (order, acts, keys, values, logits, *states)
    return pl.pallas_call(
        functools.partial(kernel, n_inst, n_rep),
        out_shape=tuple(jax.ShapeDtypeStruct(s.shape, s.dtype) for s in states),
        in_specs=[pl.BlockSpec(memory_space=pltpu.HBM)] * len(operands),
        out_specs=(vmem,) * len(states),
        scratch_shapes=scratch,
        compiler_params=pltpu.CompilerParams(
            collective_id=0, has_side_effects=True, vmem_limit_bytes=VMEM_BYTES
        ),
        cost_estimate=pl.CostEstimate(
            flops=4 * acts.shape[0] * acts.shape[1] * kv,
            bytes_accessed=24 * 2**20,
            transcendentals=0,
        ),
    )(*[pltpu.with_memory_space_constraint(x, pltpu.HBM) for x in operands])


def write_kernel(*refs):
    many = (len(refs) - 1) // 2
    copies = [
        pltpu.make_async_copy(refs[at], refs[many + at], refs[-1].at[at]) for at in range(many)
    ]
    for copy in copies:
        copy.start()
    for copy in copies:
        copy.wait()


def written(arrays):
    return pl.pallas_call(
        write_kernel,
        out_shape=tuple(jax.ShapeDtypeStruct(a.shape, a.dtype) for a in arrays),
        in_specs=[pl.BlockSpec(memory_space=pl.ANY)] * len(arrays),
        out_specs=(pl.BlockSpec(memory_space=pltpu.HBM),) * len(arrays),
        scratch_shapes=[pltpu.SemaphoreType.DMA((len(arrays),))],
        compiler_params=pltpu.CompilerParams(vmem_limit_bytes=2**20),
        cost_estimate=pl.CostEstimate(flops=2**20, bytes_accessed=24 * 2**20, transcendentals=0),
    )(*arrays)


def on_device(n_inst, n_rep, acts, grad_keys, grad_values, grad_logits, order, *states):
    fresh = summed(order, acts, grad_keys, grad_values, grad_logits, states, n_inst, n_rep)
    return written(fresh)


def solution(mesh):
    return jax.shard_map(
        functools.partial(on_device, mesh.shape["inst"], mesh.shape["rep"]),
        mesh=mesh,
        in_specs=(
            P(("rep", "inst"), None),
            P(("rep", "inst"), None),
            P(("rep", "inst"), None),
            P(None, ("rep", "inst")),
            P(),
            P(None, "inst", None),
            P(None, "inst", None),
            P(None, "inst", None),
            P("inst", None),
            P("inst", None),
            P("inst", None),
        ),
        out_specs=(
            P(None, "inst", None),
            P(None, "inst", None),
            P(None, "inst", None),
            P("inst", None),
            P("inst", None),
            P("inst", None),
        ),
        check_vma=False,
    )
```

```python
import functools

import jax
import jax.numpy as jnp
from jax import lax
from jax.experimental import pallas as pl
from jax.experimental.pallas import tpu as pltpu
from jax.sharding import PartitionSpec as P

MESH = pl.DeviceIdType.MESH
BUCKETS = 4
BLOCK_ROWS = 256
COLS = 128
SPLIT = 4
LAG = 4
HOP = 4
NEAR = 16
FAR = 32
SIGNALS = 16
FRONT = 10
FRONT_TWO = 0
ROUTER_START = 10
VMEM_BYTES = 36 * 2**20


beta_first = 0.9
beta_second = 0.95
step_rate = 0.05
decay_rate = 0.1
epsilon = 1e-08
correct_first = 1.0 - 0.9**10
correct_second = 1.0 - 0.95**10


def adamw(grad, param, moment, second):
    moment_new = beta_first * moment + (1.0 - beta_first) * grad
    second_new = beta_second * second + (1.0 - beta_second) * grad * grad
    ratio = moment_new / correct_first / (jnp.sqrt(second_new / correct_second) + epsilon)
    param_new = param - step_rate * (ratio + decay_rate * param)
    return (param_new, moment_new, second_new)


def both(*terms):
    return functools.reduce(jnp.logical_and, terms)


def whole_part(p):
    return lax.div(p, SPLIT), lax.rem(p, SPLIT)


def is_mixed(chunk, turn):
    last = both(turn == SPLIT - 1, jnp.logical_or(chunk < FRONT, lax.rem(chunk, 2) == 0))
    if FRONT_TWO:
        last = jnp.logical_or(last, both(turn == SPLIT - 2, chunk < FRONT_TWO))
    return last


MIXED_TURNS = (SPLIT - 2, SPLIT - 1) if FRONT_TWO else (SPLIT - 1,)


class Place:
    def __init__(self, n_inst, n_rep):
        self.n_inst, self.n_rep = n_inst, n_rep
        self.bits = n_inst.bit_length() - 1
        self.me, self.rep = lax.axis_index("inst"), lax.axis_index("rep")
        self.left = n_rep // 2 - 1
        low = self.rep <= self.left
        self.depth = jnp.where(low, self.rep, n_rep - 1 - self.rep)
        way = jnp.where(low, 1, -1)
        self.inner, self.outer = self.rep + way, self.rep - way
        self.flips = [(1 - 2 * ((self.me // 2**bit) % 2)) * 2**bit for bit in range(self.bits)]
        self.mixes = n_rep >= 4
        self.mate = jnp.where(self.depth == 0, self.inner, self.outer)
        self.edge = self.depth <= 1
        self.base = 1 + LAG * (self.bits - 1)
        self.top = self.base + HOP * (self.left + 1)
        self.last_step = self.top + HOP * self.left


class Lane:
    def __init__(self, place, kind, dims, refs, sems, signals, finish):
        self.place, self.kind, self.dims = place, kind, dims
        self.parts, self.halves, self.outs, self.ins, self.raws = refs
        self.send, self.recv, self.raw_send, self.raw_recv = sems
        self.finish = finish
        self.stages = len(dims)
        self.signals = signals

    def owner(self, q):
        index = self.place.me
        for at, bit in enumerate(self.dims):
            flip = lax.rem(lax.div(q, 2 ** (self.stages - 1 - at)), 2)
            index = index + flip * self.place.flips[bit]
        return index

    def half_copy(self, stage, p):
        count = self.place.n_inst >> (stage + 1)
        source = self.parts(p) if stage == 0 else self.halves(stage - 1, p)
        return pltpu.make_async_remote_copy(
            src_ref=source.at[pl.ds(count, count)],
            dst_ref=self.halves(stage, p),
            send_sem=self.send.at[stage, lax.rem(p, self.signals)],
            recv_sem=self.recv.at[stage, lax.rem(p, self.signals)],
            device_id={"inst": self.place.me + self.place.flips[self.dims[stage]]},
            device_id_type=MESH,
        )

    def arrive(self, stage, p):
        self.half_copy(stage, p).wait()
        count = self.place.n_inst >> (stage + 1)
        source = self.parts(p) if stage == 0 else self.halves(stage - 1, p)
        into = self.halves(stage, p)
        into[...] += source[pl.ds(0, count)]

    def raw_copy(self, p, at):
        return pltpu.make_async_remote_copy(
            src_ref=self.halves(0, p),
            dst_ref=self.raws(at),
            send_sem=self.raw_send.at[at],
            recv_sem=self.raw_recv.at[at],
            device_id={"rep": self.place.mate},
            device_id_type=MESH,
        )

    def total(self, p):
        return self.halves(self.stages - 1, p)

    def inward(self, p, middle):
        return pltpu.make_async_remote_copy(
            src_ref=self.total(p),
            dst_ref=self.ins(p) if middle else self.outs(p),
            send_sem=self.send.at[self.stages, lax.rem(p, self.signals)],
            recv_sem=self.recv.at[
                self.stages + 1 if middle else self.stages, lax.rem(p, self.signals)
            ],
            device_id={"rep": self.place.inner},
            device_id_type=MESH,
        )

    def outward(self, p):
        return pltpu.make_async_remote_copy(
            src_ref=self.ins(p),
            dst_ref=self.ins(p),
            send_sem=self.send.at[self.stages + 1, lax.rem(p, self.signals)],
            recv_sem=self.recv.at[self.stages + 1, lax.rem(p, self.signals)],
            device_id={"rep": self.place.outer},
            device_id_type=MESH,
        )


def begin(place, lanes, p, mixes):
    advance(place, lanes, jnp.int32(p), p + 1, mixes, only_start=True)


def advance(place, lanes, t, count, mixes, least=0, only_start=False):
    mixes = mixes and place.mixes

    def due(lag, body):
        p = t - lag

        @pl.when(both(p >= 0, p < count))
        def _():
            body(p)

    def odd(lane, chunk, turn):
        return lax.rem(chunk + turn + lane.kind + place.depth, 2) == 1

    def each_lane(body):
        for lane in lanes:
            body(lane)

    def raw_at(chunk, turn):
        return chunk if turn == SPLIT - 1 else count // SPLIT + chunk

    def mixed(p, body):
        chunk, turn = whole_part(p)
        for fixed in MIXED_TURNS:

            @pl.when(both(turn == fixed, is_mixed(chunk, fixed)))
            def _():
                for lane in lanes:
                    takes = odd(lane, chunk, fixed)
                    body(lane, chunk, fixed, takes)

    def early(p, body):
        chunk, turn = whole_part(p)

        @pl.when(turn == 0)
        def _():
            for fixed in MIXED_TURNS:

                @pl.when(is_mixed(chunk, fixed))
                def _():
                    for lane in lanes:
                        body(lane, p + fixed, chunk, fixed)

    def plain(p, body):
        if not mixes:
            each_lane(body)
            return
        chunk, turn = whole_part(p)

        @pl.when(jnp.logical_not(is_mixed(chunk, turn)))
        def _():
            each_lane(body)

    def start(p):
        plain(p, lambda lane: lane.half_copy(0, p).start())
        if mixes:
            early(p, lambda lane, at, chunk, turn: lane.half_copy(0, at).start())

    if only_start:
        start(t)
        return

    @pl.when(both(t >= least, t < count))
    def _():
        start(t)

    def onward(lane, p):
        if place.bits > 1:
            lane.half_copy(1, p).start()

    def first(p):
        def usual(lane):
            lane.arrive(0, p)
            onward(lane, p)

        plain(p, usual)
        if not mixes:
            return

        def taken(lane, chunk, turn, takes):
            at = raw_at(chunk, turn)

            @pl.when(both(place.edge, takes))
            def _():
                lane.raw_copy(p, at).wait_recv()
                into = lane.halves(0, p)
                into[...] += lane.raws(at)[...]

            @pl.when(jnp.logical_or(jnp.logical_not(place.edge), takes))
            def _():
                onward(lane, p)

        mixed(p, taken)

        def given(lane, p, chunk, turn):
            lane.arrive(0, p)

            @pl.when(both(place.edge, jnp.logical_not(odd(lane, chunk, turn))))
            def _():
                lane.raw_copy(p, raw_at(chunk, turn)).start()

        early(p, given)

    due(1, first)

    def later(stage):
        def usual(lane, p):
            lane.arrive(stage, p)
            if stage < place.bits - 1:
                lane.half_copy(stage + 1, p).start()
            else:

                @pl.when(place.depth == 0)
                def _():
                    lane.inward(p, place.left == 0).start()

        def body(p):
            plain(p, lambda lane: usual(lane, p))
            if not mixes:
                return

            def special(lane, chunk, turn, takes):
                gives = both(place.edge, jnp.logical_not(takes))

                @pl.when(jnp.logical_not(gives))
                def _():
                    usual(lane, p)

                if stage == 1:

                    @pl.when(gives)
                    def _():
                        lane.raw_copy(p, raw_at(chunk, turn)).wait_send()

            mixed(p, special)

        return body

    for stage in range(1, place.bits):
        due(1 + LAG * stage, later(stage))

    def collect(p):
        def go(lane):
            if place.left == 1:
                lane.inward(p, True).start()
            else:
                for middle in (False, True):

                    @pl.when((place.depth == place.left) == middle)
                    def _():
                        lane.inward(p, middle).start()

        def usual(lane):
            lane.inward(p, False).wait_recv()
            into = lane.total(p)
            into[...] += lane.outs(p)[...]
            go(lane)

        def special(lane, chunk, turn, takes):
            near = place.depth == 1

            @pl.when(both(near, jnp.logical_not(takes)))
            def _():
                lane.inward(p, False).wait_recv()
                lane.total(p)[...] = lane.outs(p)[...]

            @pl.when(jnp.logical_not(near))
            def _():
                lane.inward(p, False).wait_recv()
                into = lane.total(p)
                into[...] += lane.outs(p)[...]

            go(lane)

        @pl.when(place.depth > 0)
        def _():
            plain(p, usual)
            if mixes:
                mixed(p, special)

    if place.left > 0:
        due(place.base + HOP * place.depth, collect)

    def share(p):
        for lane in lanes:
            lane.outward(p).wait_recv()

            @pl.when(place.depth == place.left)
            def _(lane=lane):
                into = lane.ins(p)
                into[...] += lane.total(p)[...]

            @pl.when(place.depth > 0)
            def _(lane=lane):
                lane.outward(p).start()

        for lane in lanes:
            lane.finish(p)

    due(place.top + HOP * (place.left - place.depth), share)

    def settle(p):
        def sent(lane):
            lane.inward(p, False).wait_send()

        plain(p, sent)
        if mixes:

            def special(lane, chunk, turn, takes):
                @pl.when(jnp.logical_or(place.depth > 0, takes))
                def _():
                    sent(lane)

            mixed(p, special)

        @pl.when(place.depth > 0)
        def _():
            for lane in lanes:
                lane.outward(p).wait_send()

    due(place.last_step, settle)


def kernel(n_inst, n_rep, *refs):
    order_in, acts, keys_in, values_in, logits_in = refs[:5]
    state_in, state = refs[5:11], refs[11:17]
    order, slabs, keys, values, logits, turned, router_all, parts, router_parts = refs[17:26]
    raws, load = refs[26:28]
    scratch = refs[28:]
    place = Place(n_inst, n_rep)
    bits, rep = place.bits, place.rep
    rows = slabs.shape[-1]
    width = router_parts.shape[-1]
    per_bucket = order.shape[0] // BUCKETS
    column_blocks = acts.shape[1] // BLOCK_ROWS
    chunks = keys.shape[1] // COLS
    every = chunks * BUCKETS // 2
    count = every * SPLIT
    size = COLS // SPLIT
    halves = scratch[:bits]
    router_halves = scratch[bits : 2 * bits]
    outs, ins, router_outs, router_ins = scratch[2 * bits : 2 * bits + 4]
    sends, recvs, router_sends, router_recvs, raw_sends, raw_recvs = scratch[2 * bits + 4 :]

    def finish(kind):
        def body(p):
            chunk, turn = whole_part(p)

            @pl.when(turn == SPLIT - 1)
            def _():
                bucket = 2 * lax.div(chunk, chunks) + kind
                start = pl.multiple_of(lax.rem(chunk, chunks) * COLS, COLS)
                slot = lax.rem(chunk * SPLIT, ins.shape[1])
                grad = ins[kind, pl.ds(slot, SPLIT), 0].reshape(COLS, rows).T
                at = (bucket, slice(None), pl.ds(start, COLS))
                fresh = adamw(grad, *[part[at] for part in state[:3]])
                for part, value in zip(state[:3], fresh):
                    part[at] = value

        return body

    def router_finish(p):
        line = state[3].shape[1]
        for at in range(state[3].shape[0]):
            one = (pl.ds(at, 1), slice(None))
            grad = router_ins[0, :, pl.ds(at * line, line)]
            fresh = adamw(grad, *[part[one] for part in state[3:]])
            for part, value in zip(state[3:], fresh):
                part[one] = value

    forward = [0] + list(range(1, bits))
    backward = [0] + list(range(bits - 1, 0, -1))
    lanes = []
    for kind, dims in enumerate((forward, backward)):
        lanes.append(
            Lane(
                place,
                kind,
                dims,
                (
                    lambda p, kind=kind: parts.at[kind, lax.rem(p, 2 * SPLIT)],
                    lambda stage, p, kind=kind: halves[stage].at[
                        kind, lax.rem(p, halves[stage].shape[1])
                    ],
                    lambda p, kind=kind: outs.at[kind, lax.rem(p, outs.shape[1])],
                    lambda p, kind=kind: ins.at[kind, lax.rem(p, ins.shape[1])],
                    lambda at: raws.at[at],
                ),
                (sends.at[kind], recvs.at[kind], raw_sends, raw_recvs),
                SIGNALS,
                finish(kind),
            )
        )
    router = Lane(
        place,
        0,
        forward,
        (
            lambda p: router_parts,
            lambda stage, p: router_halves[stage],
            lambda p: router_outs,
            lambda p: router_ins,
            None,
        ),
        (router_sends, router_recvs, None, None),
        1,
        router_finish,
    )

    lead, rest = pl.ds(0, COLS), pl.ds(COLS, keys.shape[1] - COLS)
    early = [(order_in, order)]
    early += [(keys_in.at[:, lead], keys.at[:, lead]), (values_in.at[:, lead], values.at[:, lead])]
    early += [
        (acts.at[:, pl.ds(at * rows, rows)], slabs.at[at]) for at in range(slabs.shape[0])
    ]
    late = [(keys_in.at[:, rest], keys.at[:, rest]), (values_in.at[:, rest], values.at[:, rest])]
    late += [(logits_in, logits)]
    late += list(zip(state_in, state))
    loads = [
        pltpu.make_async_copy(src, dst, load.at[at]) for at, (src, dst) in enumerate(early + late)
    ]
    early, late, states = loads[: len(early)], loads[len(early) : -len(state)], loads[-len(state) :]
    for copy in early + late:
        copy.start()

    barrier = pltpu.get_barrier_semaphore()
    for flip in place.flips:
        pl.semaphore_signal(
            barrier, inc=1, device_id={"inst": place.me + flip}, device_id_type=MESH
        )

    @pl.when(rep > 0)
    def _():
        pl.semaphore_signal(barrier, inc=1, device_id={"rep": rep - 1}, device_id_type=MESH)

    @pl.when(rep < n_rep - 1)
    def _():
        pl.semaphore_signal(barrier, inc=1, device_id={"rep": rep + 1}, device_id_type=MESH)

    for copy in early:
        copy.wait()

    each = n_inst // SPLIT

    def turn_over(chunk):
        column = pl.multiple_of(lax.rem(chunk, chunks) * COLS, COLS)
        turned[0] = keys[:, pl.ds(column, COLS)].T
        turned[1] = values[:, pl.ds(column, COLS)].T

    def products(chunk, turn):
        slot = lax.rem(chunk, 2) * SPLIT
        for kind, lane in enumerate(lanes):
            bucket = 2 * lax.div(chunk, chunks) + kind
            for i in range(each):
                q = turn * each + i
                first = lane.owner(q) * rows
                block = order[bucket * per_bucket + lax.div(first, BLOCK_ROWS)]
                at = lax.rem(block, column_blocks) * (BLOCK_ROWS // rows)
                at = at + lax.div(lax.rem(first, BLOCK_ROWS), rows)
                full = jnp.dot(
                    turned[lax.div(block, column_blocks)],
                    slabs[at],
                    preferred_element_type=jnp.float32,
                )
                for part in range(SPLIT):
                    parts[kind, slot + part, q] = full[part * size : (part + 1) * size]

    def router_products():
        for at in range(slabs.shape[0]):
            router_all[:, pl.ds(at * rows, rows)] = jnp.dot(
                logits[...], slabs[at], preferred_element_type=jnp.float32
            )
        for q in range(n_inst):
            first = router.owner(q) * width
            router_parts[q] = router_all[
                pl.ds(first // acts.shape[1], 1),
                pl.ds(pl.multiple_of(first % acts.shape[1], width), width),
            ]

    def head(turn, carry):
        products(0, turn)
        return carry

    turn_over(0)
    lax.fori_loop(SPLIT // 2, SPLIT, head, 0)
    peers = bits + jnp.where(rep > 0, 1, 0) + jnp.where(rep < n_rep - 1, 1, 0)
    pl.semaphore_wait(barrier, peers)
    begin(place, lanes, 0, True)
    lax.fori_loop(0, SPLIT // 2, head, 0)
    for copy in states:
        copy.start()
    for copy in late:
        copy.wait()

    def step(t, carry):
        advance(place, lanes, t, count, True, least=1)

        @pl.when(t == ROUTER_START)
        def _():
            router_products()
            for copy in states:
                copy.wait()

        @pl.when(both(t >= ROUTER_START, t <= ROUTER_START + place.last_step))
        def _():
            advance(place, [router], t - ROUTER_START, 1, False)

        @pl.when(t < count - SPLIT)
        def _():
            chunk, turn = lax.div(t, SPLIT) + 1, lax.rem(t, SPLIT)

            @pl.when(turn == 0)
            def _():
                turn_over(chunk)

            products(chunk, turn)

        return carry

    lax.fori_loop(0, count + place.last_step, step, 0)


def summed(order, acts, keys, values, logits, states, n_inst, n_rep):
    bits = n_inst.bit_length() - 1
    rows = states[0].shape[1]
    width = states[3].size
    kv = keys.shape[1]
    size = COLS // SPLIT
    every = kv // COLS * BUCKETS // 2
    count = every * SPLIT
    vmem = pl.BlockSpec(memory_space=pltpu.VMEM)
    f32 = jnp.float32
    scratch = [
        pltpu.SMEM(order.shape, order.dtype),
        pltpu.VMEM((acts.shape[1] // rows, acts.shape[0], rows), acts.dtype),
        pltpu.VMEM(keys.shape, keys.dtype),
        pltpu.VMEM(values.shape, values.dtype),
        pltpu.VMEM(logits.shape, logits.dtype),
        pltpu.VMEM((2, COLS, acts.shape[0]), acts.dtype),
        pltpu.VMEM((logits.shape[0], acts.shape[1]), f32),
        pltpu.VMEM((2, 2 * SPLIT, n_inst, size, rows), f32),
        pltpu.VMEM((n_inst, 1, width), f32),
        pltpu.VMEM((every + FRONT_TWO, n_inst // 2, size, rows), f32),
        pltpu.SemaphoreType.DMA((acts.shape[1] // rows + 6 + len(states),)),
    ]
    scratch += [
        pltpu.VMEM((2, min(count, FAR if s else NEAR), n_inst >> (s + 1), size, rows), f32)
        for s in range(bits)
    ]
    scratch += [pltpu.VMEM((n_inst >> (s + 1), 1, width), f32) for s in range(bits)]
    scratch += [pltpu.VMEM((2, min(count, FAR), 1, size, rows), f32)] * 2
    scratch += [pltpu.VMEM((1, 1, width), f32)] * 2
    scratch += [pltpu.SemaphoreType.DMA((2, bits + 2, SIGNALS))] * 2
    scratch += [pltpu.SemaphoreType.DMA((bits + 2, 1))] * 2
    scratch += [pltpu.SemaphoreType.DMA((every + FRONT_TWO,))] * 2
    operands = (order, acts, keys, values, logits, *states)
    return pl.pallas_call(
        functools.partial(kernel, n_inst, n_rep),
        out_shape=tuple(jax.ShapeDtypeStruct(s.shape, s.dtype) for s in states),
        in_specs=[pl.BlockSpec(memory_space=pltpu.HBM)] * len(operands),
        out_specs=(vmem,) * len(states),
        scratch_shapes=scratch,
        compiler_params=pltpu.CompilerParams(
            collective_id=0, has_side_effects=True, vmem_limit_bytes=VMEM_BYTES
        ),
        cost_estimate=pl.CostEstimate(
            flops=4 * acts.shape[0] * acts.shape[1] * kv,
            bytes_accessed=24 * 2**20,
            transcendentals=0,
        ),
    )(*[pltpu.with_memory_space_constraint(x, pltpu.HBM) for x in operands])


def write_kernel(*refs):
    many = (len(refs) - 1) // 2
    copies = [
        pltpu.make_async_copy(refs[at], refs[many + at], refs[-1].at[at]) for at in range(many)
    ]
    for copy in copies:
        copy.start()
    for copy in copies:
        copy.wait()


def written(arrays):
    return pl.pallas_call(
        write_kernel,
        out_shape=tuple(jax.ShapeDtypeStruct(a.shape, a.dtype) for a in arrays),
        in_specs=[pl.BlockSpec(memory_space=pl.ANY)] * len(arrays),
        out_specs=(pl.BlockSpec(memory_space=pltpu.HBM),) * len(arrays),
        scratch_shapes=[pltpu.SemaphoreType.DMA((len(arrays),))],
        compiler_params=pltpu.CompilerParams(vmem_limit_bytes=2**20),
        cost_estimate=pl.CostEstimate(flops=2**20, bytes_accessed=24 * 2**20, transcendentals=0),
    )(*arrays)


def on_device(n_inst, n_rep, acts, grad_keys, grad_values, grad_logits, order, *states):
    fresh = summed(order, acts, grad_keys, grad_values, grad_logits, states, n_inst, n_rep)
    return written(fresh)


def solution(mesh):
    return jax.shard_map(
        functools.partial(on_device, mesh.shape["inst"], mesh.shape["rep"]),
        mesh=mesh,
        in_specs=(
            P(("rep", "inst"), None),
            P(("rep", "inst"), None),
            P(("rep", "inst"), None),
            P(None, ("rep", "inst")),
            P(),
            P(None, "inst", None),
            P(None, "inst", None),
            P(None, "inst", None),
            P("inst", None),
            P("inst", None),
            P("inst", None),
        ),
        out_specs=(
            P(None, "inst", None),
            P(None, "inst", None),
            P(None, "inst", None),
            P("inst", None),
            P("inst", None),
            P("inst", None),
        ),
        check_vma=False,
    )
```

```python
import functools

import jax
import jax.numpy as jnp
from jax import lax
from jax.experimental import pallas as pl
from jax.experimental.pallas import tpu as pltpu
from jax.sharding import PartitionSpec as P

MESH = pl.DeviceIdType.MESH
BUCKETS = 4
BLOCK_ROWS = 256
COLS = 128
SPLIT = 4
LAG = 3
HOP = 3
NEAR = 16
FAR = 32
SIGNALS = 12
ENDS = 14
BACK = 2
MIDDLE = 12
RAW = 4
ROUTER_START = 10
VMEM_BYTES = 36 * 2**20


beta_first = 0.9
beta_second = 0.95
step_rate = 0.05
decay_rate = 0.1
epsilon = 1e-08
correct_first = 1.0 - 0.9**10
correct_second = 1.0 - 0.95**10


def adamw(grad, param, moment, second):
    moment_new = beta_first * moment + (1.0 - beta_first) * grad
    second_new = beta_second * second + (1.0 - beta_second) * grad * grad
    ratio = moment_new / correct_first / (jnp.sqrt(second_new / correct_second) + epsilon)
    param_new = param - step_rate * (ratio + decay_rate * param)
    return (param_new, moment_new, second_new)


def both(*terms):
    return functools.reduce(jnp.logical_and, terms)


def whole_part(p):
    return lax.div(p, SPLIT), lax.rem(p, SPLIT)


def in_ends(chunk):
    return chunk < ENDS


def in_middle(chunk):
    return jnp.logical_or(chunk < 4, both(lax.rem(chunk, 2) == 1, chunk < MIDDLE))


def is_mixed(chunk, turn):
    return jnp.logical_or(
        both(turn == SPLIT - 1, in_ends(chunk)), both(turn == SPLIT - 2, in_middle(chunk))
    )


MIXED_TURNS = (SPLIT - 1, SPLIT - 2)


class Place:
    def __init__(self, n_inst, n_rep):
        self.n_inst, self.n_rep = n_inst, n_rep
        self.bits = n_inst.bit_length() - 1
        self.me, self.rep = lax.axis_index("inst"), lax.axis_index("rep")
        self.left = n_rep // 2 - 1
        low = self.rep <= self.left
        self.depth = jnp.where(low, self.rep, n_rep - 1 - self.rep)
        way = jnp.where(low, 1, -1)
        self.inner, self.outer = self.rep + way, self.rep - way
        self.flips = [(1 - 2 * ((self.me // 2**bit) % 2)) * 2**bit for bit in range(self.bits)]
        self.mixes = n_rep >= 4
        self.mate = jnp.where(self.depth == 0, self.inner, self.outer)
        self.side = jnp.where(low, 0, 1)
        self.base = 1 + LAG * (self.bits - 1)
        self.top = self.base + HOP * (self.left + 1)
        self.last_step = self.top + HOP * self.left


class Lane:
    def __init__(self, place, kind, dims, refs, sems, signals, finish):
        self.place, self.kind, self.dims = place, kind, dims
        self.parts, self.halves, self.outs, self.ins, self.raws = refs
        self.send, self.recv, self.raw_send, self.raw_recv = sems
        self.finish = finish
        self.stages = len(dims)
        self.signals = signals

    def owner(self, q):
        index = self.place.me
        for at, bit in enumerate(self.dims):
            flip = lax.rem(lax.div(q, 2 ** (self.stages - 1 - at)), 2)
            index = index + flip * self.place.flips[bit]
        return index

    def half_copy(self, stage, p):
        count = self.place.n_inst >> (stage + 1)
        source = self.parts(p) if stage == 0 else self.halves(stage - 1, p)
        return pltpu.make_async_remote_copy(
            src_ref=source.at[pl.ds(count, count)],
            dst_ref=self.halves(stage, p),
            send_sem=self.send.at[stage, lax.rem(p, self.signals)],
            recv_sem=self.recv.at[stage, lax.rem(p, self.signals)],
            device_id={"inst": self.place.me + self.place.flips[self.dims[stage]]},
            device_id_type=MESH,
        )

    def arrive(self, stage, p):
        self.half_copy(stage, p).wait()
        count = self.place.n_inst >> (stage + 1)
        source = self.parts(p) if stage == 0 else self.halves(stage - 1, p)
        into = self.halves(stage, p)
        into[...] += source[pl.ds(0, count)]

    def role(self, chunk, turn):
        depth = self.place.depth
        if turn == SPLIT - 1:
            inward = lax.rem(chunk + self.kind, 2) == 0
            outward = both(jnp.logical_not(inward), lax.rem(lax.div(chunk, 2), BACK) == 0)
            end, near = depth == 0, depth == 1
            gives = jnp.logical_or(both(inward, end), both(outward, near))
            takes = jnp.logical_or(both(inward, near), both(outward, end))
            return gives, takes, both(inward, near)
        middle = depth == self.place.left
        even = lax.rem(chunk + self.kind + self.place.side, 2) == 0
        return both(middle, even), both(middle, jnp.logical_not(even)), depth < 0

    def raw_copy(self, p, chunk, turn):
        at = lax.rem(chunk, RAW) + (RAW if turn == SPLIT - 2 else 0)
        return pltpu.make_async_remote_copy(
            src_ref=self.halves(0, p),
            dst_ref=self.raws(at),
            send_sem=self.raw_send.at[at],
            recv_sem=self.raw_recv.at[at],
            device_id={"rep": self.place.mate if turn == SPLIT - 1 else self.place.inner},
            device_id_type=MESH,
        )

    def total(self, p):
        return self.halves(self.stages - 1, p)

    def inward(self, p, middle):
        return pltpu.make_async_remote_copy(
            src_ref=self.total(p),
            dst_ref=self.ins(p) if middle else self.outs(p),
            send_sem=self.send.at[self.stages, lax.rem(p, self.signals)],
            recv_sem=self.recv.at[
                self.stages + 1 if middle else self.stages, lax.rem(p, self.signals)
            ],
            device_id={"rep": self.place.inner},
            device_id_type=MESH,
        )

    def outward(self, p):
        return pltpu.make_async_remote_copy(
            src_ref=self.ins(p),
            dst_ref=self.ins(p),
            send_sem=self.send.at[self.stages + 1, lax.rem(p, self.signals)],
            recv_sem=self.recv.at[self.stages + 1, lax.rem(p, self.signals)],
            device_id={"rep": self.place.outer},
            device_id_type=MESH,
        )


def begin(place, lanes, p, mixes):
    advance(place, lanes, jnp.int32(p), p + 1, mixes, only_start=True)


def advance(place, lanes, t, count, mixes, least=0, only_start=False):
    mixes = mixes and place.mixes

    def due(lag, body):
        p = t - lag

        @pl.when(both(p >= 0, p < count))
        def _():
            body(p)

    def each_lane(body):
        for lane in lanes:
            body(lane)

    def mixed(p, body):
        chunk, turn = whole_part(p)
        for fixed in MIXED_TURNS:

            @pl.when(both(turn == fixed, is_mixed(chunk, fixed)))
            def _():
                for lane in lanes:
                    body(lane, p, chunk, fixed, *lane.role(chunk, fixed))

    def together(p, body):
        chunk, turn = whole_part(p)

        @pl.when(turn == SPLIT - 1)
        def _():
            for fixed in MIXED_TURNS:

                @pl.when(is_mixed(chunk, fixed))
                def _():
                    for lane in lanes:
                        at = p + fixed - SPLIT + 1
                        body(lane, at, chunk, fixed, *lane.role(chunk, fixed))

    def early(p, body):
        chunk, turn = whole_part(p)

        @pl.when(turn == 0)
        def _():
            for fixed in MIXED_TURNS:

                @pl.when(is_mixed(chunk, fixed))
                def _():
                    for lane in lanes:
                        body(lane, p + fixed, chunk, fixed)

    def plain(p, body):
        if not mixes:
            each_lane(body)
            return
        chunk, turn = whole_part(p)

        @pl.when(jnp.logical_not(is_mixed(chunk, turn)))
        def _():
            each_lane(body)

    def start(p):
        plain(p, lambda lane: lane.half_copy(0, p).start())
        if mixes:
            early(p, lambda lane, at, chunk, turn: lane.half_copy(0, at).start())

    if only_start:
        start(t)
        return

    @pl.when(both(t >= least, t < count))
    def _():
        start(t)

    def onward(lane, p):
        if place.bits > 1:
            lane.half_copy(1, p).start()

    def first(p):
        def usual(lane):
            lane.arrive(0, p)
            onward(lane, p)

        plain(p, usual)
        if not mixes:
            return

        def taken(lane, p, chunk, turn, gives, takes, misses):
            @pl.when(takes)
            def _():
                lane.raw_copy(p, chunk, turn).wait_recv()
                into = lane.halves(0, p)
                into[...] += lane.raws(lax.rem(chunk, RAW) + (RAW if turn == SPLIT - 2 else 0))[...]

            @pl.when(jnp.logical_not(gives))
            def _():
                onward(lane, p)

        together(p, taken)

        def given(lane, p, chunk, turn):
            lane.arrive(0, p)

            @pl.when(lane.role(chunk, turn)[0])
            def _():
                lane.raw_copy(p, chunk, turn).start()

        early(p, given)

    due(1, first)

    def later(stage):
        def usual(lane, p):
            lane.arrive(stage, p)
            if stage < place.bits - 1:
                lane.half_copy(stage + 1, p).start()
            else:

                @pl.when(place.depth == 0)
                def _():
                    lane.inward(p, place.left == 0).start()

        def body(p):
            plain(p, lambda lane: usual(lane, p))
            if not mixes:
                return

            def special(lane, p, chunk, turn, gives, takes, misses):
                @pl.when(jnp.logical_not(gives))
                def _():
                    usual(lane, p)

                if stage == 1:

                    @pl.when(gives)
                    def _():
                        lane.raw_copy(p, chunk, turn).wait_send()

            mixed(p, special)

        return body

    for stage in range(1, place.bits):
        due(1 + LAG * stage, later(stage))

    def collect(p):
        def go(lane):
            if place.left == 1:
                lane.inward(p, True).start()
            else:
                for middle in (False, True):

                    @pl.when((place.depth == place.left) == middle)
                    def _():
                        lane.inward(p, middle).start()

        def usual(lane):
            lane.inward(p, False).wait_recv()
            into = lane.total(p)
            into[...] += lane.outs(p)[...]
            go(lane)

        def special(lane, p, chunk, turn, gives, takes, misses):
            @pl.when(gives)
            def _():
                lane.inward(p, False).wait_recv()
                lane.total(p)[...] = lane.outs(p)[...]

            @pl.when(jnp.logical_not(jnp.logical_or(gives, misses)))
            def _():
                lane.inward(p, False).wait_recv()
                into = lane.total(p)
                into[...] += lane.outs(p)[...]

            go(lane)

        @pl.when(place.depth > 0)
        def _():
            plain(p, usual)
            if mixes:
                mixed(p, special)

    if place.left > 0:
        due(place.base + HOP * place.depth, collect)

    def share(p):
        for lane in lanes:
            lane.outward(p).wait_recv()

            @pl.when(place.depth == place.left)
            def _(lane=lane):
                into = lane.ins(p)
                into[...] += lane.total(p)[...]

            @pl.when(place.depth > 0)
            def _(lane=lane):
                lane.outward(p).start()

        for lane in lanes:
            lane.finish(p)

    due(place.top + HOP * (place.left - place.depth), share)

    def settle(p):
        def sent(lane):
            lane.inward(p, False).wait_send()

        plain(p, sent)
        if mixes:

            def special(lane, p, chunk, turn, gives, takes, misses):
                @pl.when(jnp.logical_or(place.depth > 0, jnp.logical_not(gives)))
                def _():
                    sent(lane)

            mixed(p, special)

        @pl.when(place.depth > 0)
        def _():
            for lane in lanes:
                lane.outward(p).wait_send()

    due(place.last_step, settle)


def kernel(n_inst, n_rep, *refs):
    order_in, acts, keys_in, values_in, logits_in = refs[:5]
    state_in, state = refs[5:11], refs[11:17]
    order, slabs, keys, values, logits, turned, router_all, parts, router_parts = refs[17:26]
    raws, load = refs[26:28]
    scratch = refs[28:]
    place = Place(n_inst, n_rep)
    bits, rep = place.bits, place.rep
    rows = slabs.shape[-1]
    width = router_parts.shape[-1]
    per_bucket = order.shape[0] // BUCKETS
    column_blocks = acts.shape[1] // BLOCK_ROWS
    chunks = keys.shape[1] // COLS
    every = chunks * BUCKETS // 2
    count = every * SPLIT
    size = COLS // SPLIT
    halves = scratch[:bits]
    router_halves = scratch[bits : 2 * bits]
    outs, ins, router_outs, router_ins = scratch[2 * bits : 2 * bits + 4]
    sends, recvs, router_sends, router_recvs, raw_sends, raw_recvs = scratch[2 * bits + 4 :]

    def finish(kind):
        def body(p):
            chunk, turn = whole_part(p)

            @pl.when(turn == SPLIT - 1)
            def _():
                bucket = 2 * lax.div(chunk, chunks) + kind
                start = pl.multiple_of(lax.rem(chunk, chunks) * COLS, COLS)
                slot = lax.rem(chunk * SPLIT, ins.shape[1])
                grad = ins[kind, pl.ds(slot, SPLIT), 0].reshape(COLS, rows).T
                at = (bucket, slice(None), pl.ds(start, COLS))
                fresh = adamw(grad, *[part[at] for part in state[:3]])
                for part, value in zip(state[:3], fresh):
                    part[at] = value

        return body

    def router_finish(p):
        line = state[3].shape[1]
        for at in range(state[3].shape[0]):
            one = (pl.ds(at, 1), slice(None))
            grad = router_ins[0, :, pl.ds(at * line, line)]
            fresh = adamw(grad, *[part[one] for part in state[3:]])
            for part, value in zip(state[3:], fresh):
                part[one] = value

    forward = [0] + list(range(1, bits))
    backward = [0] + list(range(bits - 1, 0, -1))
    lanes = []
    for kind, dims in enumerate((forward, backward)):
        lanes.append(
            Lane(
                place,
                kind,
                dims,
                (
                    lambda p, kind=kind: parts.at[kind, lax.rem(p, 2 * SPLIT)],
                    lambda stage, p, kind=kind: halves[stage].at[
                        kind, lax.rem(p, halves[stage].shape[1])
                    ],
                    lambda p, kind=kind: outs.at[kind, lax.rem(p, outs.shape[1])],
                    lambda p, kind=kind: ins.at[kind, lax.rem(p, ins.shape[1])],
                    lambda at: raws.at[at],
                ),
                (sends.at[kind], recvs.at[kind], raw_sends, raw_recvs),
                SIGNALS,
                finish(kind),
            )
        )
    router = Lane(
        place,
        0,
        forward,
        (
            lambda p: router_parts,
            lambda stage, p: router_halves[stage],
            lambda p: router_outs,
            lambda p: router_ins,
            None,
        ),
        (router_sends, router_recvs, None, None),
        1,
        router_finish,
    )

    lead, rest = pl.ds(0, COLS), pl.ds(COLS, keys.shape[1] - COLS)
    early = [(order_in, order)]
    early += [(keys_in.at[:, lead], keys.at[:, lead]), (values_in.at[:, lead], values.at[:, lead])]
    early += [
        (acts.at[:, pl.ds(at * rows, rows)], slabs.at[at]) for at in range(slabs.shape[0])
    ]
    late = [(keys_in.at[:, rest], keys.at[:, rest]), (values_in.at[:, rest], values.at[:, rest])]
    late += [(logits_in, logits)]
    late += list(zip(state_in, state))
    loads = [
        pltpu.make_async_copy(src, dst, load.at[at]) for at, (src, dst) in enumerate(early + late)
    ]
    early, late, states = loads[: len(early)], loads[len(early) : -len(state)], loads[-len(state) :]
    for copy in early + late:
        copy.start()

    barrier = pltpu.get_barrier_semaphore()
    for flip in place.flips:
        pl.semaphore_signal(
            barrier, inc=1, device_id={"inst": place.me + flip}, device_id_type=MESH
        )

    @pl.when(rep > 0)
    def _():
        pl.semaphore_signal(barrier, inc=1, device_id={"rep": rep - 1}, device_id_type=MESH)

    @pl.when(rep < n_rep - 1)
    def _():
        pl.semaphore_signal(barrier, inc=1, device_id={"rep": rep + 1}, device_id_type=MESH)

    for copy in early:
        copy.wait()

    each = n_inst // SPLIT

    def turn_over(chunk):
        column = pl.multiple_of(lax.rem(chunk, chunks) * COLS, COLS)
        turned[0] = keys[:, pl.ds(column, COLS)].T
        turned[1] = values[:, pl.ds(column, COLS)].T

    def products(chunk, turn):
        slot = lax.rem(chunk, 2) * SPLIT
        for kind, lane in enumerate(lanes):
            bucket = 2 * lax.div(chunk, chunks) + kind
            for i in range(each):
                q = turn * each + i
                first = lane.owner(q) * rows
                block = order[bucket * per_bucket + lax.div(first, BLOCK_ROWS)]
                at = lax.rem(block, column_blocks) * (BLOCK_ROWS // rows)
                at = at + lax.div(lax.rem(first, BLOCK_ROWS), rows)
                full = jnp.dot(
                    turned[lax.div(block, column_blocks)],
                    slabs[at],
                    preferred_element_type=jnp.float32,
                )
                for part in range(SPLIT):
                    parts[kind, slot + part, q] = full[part * size : (part + 1) * size]

    def router_products():
        for at in range(slabs.shape[0]):
            router_all[:, pl.ds(at * rows, rows)] = jnp.dot(
                logits[...], slabs[at], preferred_element_type=jnp.float32
            )
        for q in range(n_inst):
            first = router.owner(q) * width
            router_parts[q] = router_all[
                pl.ds(first // acts.shape[1], 1),
                pl.ds(pl.multiple_of(first % acts.shape[1], width), width),
            ]

    def head(turn, carry):
        products(0, turn)
        return carry

    turn_over(0)
    lax.fori_loop(SPLIT // 2, SPLIT, head, 0)
    peers = bits + jnp.where(rep > 0, 1, 0) + jnp.where(rep < n_rep - 1, 1, 0)
    pl.semaphore_wait(barrier, peers)
    begin(place, lanes, 0, True)
    lax.fori_loop(0, SPLIT // 2, head, 0)
    for copy in states:
        copy.start()
    for copy in late:
        copy.wait()

    def step(t, carry):
        advance(place, lanes, t, count, True, least=1)

        @pl.when(t == ROUTER_START)
        def _():
            router_products()
            for copy in states:
                copy.wait()

        @pl.when(both(t >= ROUTER_START, t <= ROUTER_START + place.last_step))
        def _():
            advance(place, [router], t - ROUTER_START, 1, False)

        @pl.when(t < count - SPLIT)
        def _():
            chunk, turn = lax.div(t, SPLIT) + 1, lax.rem(t, SPLIT)

            @pl.when(turn == 0)
            def _():
                turn_over(chunk)

            products(chunk, turn)

        return carry

    lax.fori_loop(0, count + place.last_step, step, 0)


def summed(order, acts, keys, values, logits, states, n_inst, n_rep):
    bits = n_inst.bit_length() - 1
    rows = states[0].shape[1]
    width = states[3].size
    kv = keys.shape[1]
    size = COLS // SPLIT
    every = kv // COLS * BUCKETS // 2
    count = every * SPLIT
    vmem = pl.BlockSpec(memory_space=pltpu.VMEM)
    f32 = jnp.float32
    scratch = [
        pltpu.SMEM(order.shape, order.dtype),
        pltpu.VMEM((acts.shape[1] // rows, acts.shape[0], rows), acts.dtype),
        pltpu.VMEM(keys.shape, keys.dtype),
        pltpu.VMEM(values.shape, values.dtype),
        pltpu.VMEM(logits.shape, logits.dtype),
        pltpu.VMEM((2, COLS, acts.shape[0]), acts.dtype),
        pltpu.VMEM((logits.shape[0], acts.shape[1]), f32),
        pltpu.VMEM((2, 2 * SPLIT, n_inst, size, rows), f32),
        pltpu.VMEM((n_inst, 1, width), f32),
        pltpu.VMEM((2 * RAW, n_inst // 2, size, rows), f32),
        pltpu.SemaphoreType.DMA((acts.shape[1] // rows + 6 + len(states),)),
    ]
    scratch += [
        pltpu.VMEM((2, min(count, FAR if s else NEAR), n_inst >> (s + 1), size, rows), f32)
        for s in range(bits)
    ]
    scratch += [pltpu.VMEM((n_inst >> (s + 1), 1, width), f32) for s in range(bits)]
    scratch += [pltpu.VMEM((2, min(count, FAR), 1, size, rows), f32)] * 2
    scratch += [pltpu.VMEM((1, 1, width), f32)] * 2
    scratch += [pltpu.SemaphoreType.DMA((2, bits + 2, SIGNALS))] * 2
    scratch += [pltpu.SemaphoreType.DMA((bits + 2, 1))] * 2
    scratch += [pltpu.SemaphoreType.DMA((2 * RAW,))] * 2
    operands = (order, acts, keys, values, logits, *states)
    return pl.pallas_call(
        functools.partial(kernel, n_inst, n_rep),
        out_shape=tuple(jax.ShapeDtypeStruct(s.shape, s.dtype) for s in states),
        in_specs=[pl.BlockSpec(memory_space=pltpu.HBM)] * len(operands),
        out_specs=(vmem,) * len(states),
        scratch_shapes=scratch,
        compiler_params=pltpu.CompilerParams(
            collective_id=0, has_side_effects=True, vmem_limit_bytes=VMEM_BYTES
        ),
        cost_estimate=pl.CostEstimate(
            flops=4 * acts.shape[0] * acts.shape[1] * kv,
            bytes_accessed=24 * 2**20,
            transcendentals=0,
        ),
    )(*[pltpu.with_memory_space_constraint(x, pltpu.HBM) for x in operands])


def write_kernel(*refs):
    many = (len(refs) - 1) // 2
    copies = [
        pltpu.make_async_copy(refs[at], refs[many + at], refs[-1].at[at]) for at in range(many)
    ]
    for copy in copies:
        copy.start()
    for copy in copies:
        copy.wait()


def written(arrays):
    return pl.pallas_call(
        write_kernel,
        out_shape=tuple(jax.ShapeDtypeStruct(a.shape, a.dtype) for a in arrays),
        in_specs=[pl.BlockSpec(memory_space=pl.ANY)] * len(arrays),
        out_specs=(pl.BlockSpec(memory_space=pltpu.HBM),) * len(arrays),
        scratch_shapes=[pltpu.SemaphoreType.DMA((len(arrays),))],
        compiler_params=pltpu.CompilerParams(vmem_limit_bytes=2**20),
        cost_estimate=pl.CostEstimate(flops=2**20, bytes_accessed=24 * 2**20, transcendentals=0),
    )(*arrays)


def on_device(n_inst, n_rep, acts, grad_keys, grad_values, grad_logits, order, *states):
    fresh = summed(order, acts, grad_keys, grad_values, grad_logits, states, n_inst, n_rep)
    return written(fresh)


def solution(mesh):
    return jax.shard_map(
        functools.partial(on_device, mesh.shape["inst"], mesh.shape["rep"]),
        mesh=mesh,
        in_specs=(
            P(("rep", "inst"), None),
            P(("rep", "inst"), None),
            P(("rep", "inst"), None),
            P(None, ("rep", "inst")),
            P(),
            P(None, "inst", None),
            P(None, "inst", None),
            P(None, "inst", None),
            P("inst", None),
            P("inst", None),
            P("inst", None),
        ),
        out_specs=(
            P(None, "inst", None),
            P(None, "inst", None),
            P(None, "inst", None),
            P("inst", None),
            P("inst", None),
            P("inst", None),
        ),
        check_vma=False,
    )
```

```python
import functools

import jax
import jax.numpy as jnp
from jax import lax
from jax.experimental import pallas as pl
from jax.experimental.pallas import tpu as pltpu
from jax.sharding import PartitionSpec as P

MESH = pl.DeviceIdType.MESH
BUCKETS = 4
BLOCK_ROWS = 256
COLS = 128
SPLIT = 4
LAG = 3
HOP = 3
NEAR = 16
FAR = 32
SIGNALS = 10
ENDS = 14
BACK = 2
MIDDLE = 12
RAW = 4
ROUTER_START = 10
VMEM_BYTES = 36 * 2**20


beta_first = 0.9
beta_second = 0.95
step_rate = 0.05
decay_rate = 0.1
epsilon = 1e-08
correct_first = 1.0 - 0.9**10
correct_second = 1.0 - 0.95**10


def adamw(grad, param, moment, second):
    moment_new = beta_first * moment + (1.0 - beta_first) * grad
    second_new = beta_second * second + (1.0 - beta_second) * grad * grad
    ratio = moment_new / correct_first / (jnp.sqrt(second_new / correct_second) + epsilon)
    param_new = param - step_rate * (ratio + decay_rate * param)
    return (param_new, moment_new, second_new)


def both(*terms):
    return functools.reduce(jnp.logical_and, terms)


def whole_part(p):
    return lax.div(p, SPLIT), lax.rem(p, SPLIT)


def in_ends(chunk):
    return chunk < ENDS


def in_middle(chunk):
    return jnp.logical_or(chunk < 4, both(lax.rem(chunk, 2) == 1, chunk < MIDDLE))


def is_mixed(chunk, turn):
    return jnp.logical_or(
        both(turn == SPLIT - 1, in_ends(chunk)), both(turn == SPLIT - 2, in_middle(chunk))
    )


MIXED_TURNS = (SPLIT - 1, SPLIT - 2)


class Place:
    def __init__(self, n_inst, n_rep):
        self.n_inst, self.n_rep = n_inst, n_rep
        self.bits = n_inst.bit_length() - 1
        self.me, self.rep = lax.axis_index("inst"), lax.axis_index("rep")
        self.left = n_rep // 2 - 1
        low = self.rep <= self.left
        self.depth = jnp.where(low, self.rep, n_rep - 1 - self.rep)
        way = jnp.where(low, 1, -1)
        self.inner, self.outer = self.rep + way, self.rep - way
        self.flips = [(1 - 2 * ((self.me // 2**bit) % 2)) * 2**bit for bit in range(self.bits)]
        self.mixes = n_rep >= 4
        self.mate = jnp.where(self.depth == 0, self.inner, self.outer)
        self.side = jnp.where(low, 0, 1)
        self.base = 1 + LAG * (self.bits - 1)
        self.top = self.base + HOP * (self.left + 1)
        self.last_step = self.top + HOP * self.left


class Lane:
    def __init__(self, place, kind, dims, refs, sems, signals, finish):
        self.place, self.kind, self.dims = place, kind, dims
        self.parts, self.halves, self.outs, self.ins, self.raws = refs
        self.send, self.recv, self.raw_send, self.raw_recv = sems
        self.finish = finish
        self.stages = len(dims)
        self.signals = signals

    def owner(self, q):
        index = self.place.me
        for at, bit in enumerate(self.dims):
            flip = lax.rem(lax.div(q, 2 ** (self.stages - 1 - at)), 2)
            index = index + flip * self.place.flips[bit]
        return index

    def half_copy(self, stage, p):
        count = self.place.n_inst >> (stage + 1)
        source = self.parts(p) if stage == 0 else self.halves(stage - 1, p)
        return pltpu.make_async_remote_copy(
            src_ref=source.at[pl.ds(count, count)],
            dst_ref=self.halves(stage, p),
            send_sem=self.send.at[stage, lax.rem(p, self.signals)],
            recv_sem=self.recv.at[stage, lax.rem(p, self.signals)],
            device_id={"inst": self.place.me + self.place.flips[self.dims[stage]]},
            device_id_type=MESH,
        )

    def arrive(self, stage, p):
        self.half_copy(stage, p).wait()
        count = self.place.n_inst >> (stage + 1)
        source = self.parts(p) if stage == 0 else self.halves(stage - 1, p)
        into = self.halves(stage, p)
        into[...] += source[pl.ds(0, count)]

    def role(self, chunk, turn):
        depth = self.place.depth
        if turn == SPLIT - 1:
            inward = lax.rem(chunk + self.kind, 2) == 0
            outward = both(jnp.logical_not(inward), lax.rem(lax.div(chunk, 2), BACK) == 0)
            end, near = depth == 0, depth == 1
            gives = jnp.logical_or(both(inward, end), both(outward, near))
            takes = jnp.logical_or(both(inward, near), both(outward, end))
            return gives, takes, both(inward, near)
        middle = depth == self.place.left
        even = lax.rem(chunk + self.kind + self.place.side, 2) == 0
        return both(middle, even), both(middle, jnp.logical_not(even)), depth < 0

    def raw_copy(self, p, chunk, turn):
        at = lax.rem(chunk, RAW) + (RAW if turn == SPLIT - 2 else 0)
        return pltpu.make_async_remote_copy(
            src_ref=self.halves(0, p),
            dst_ref=self.raws(at),
            send_sem=self.raw_send.at[at],
            recv_sem=self.raw_recv.at[at],
            device_id={"rep": self.place.mate if turn == SPLIT - 1 else self.place.inner},
            device_id_type=MESH,
        )

    def total(self, p):
        return self.halves(self.stages - 1, p)

    def inward(self, p, middle):
        return pltpu.make_async_remote_copy(
            src_ref=self.total(p),
            dst_ref=self.ins(p) if middle else self.outs(p),
            send_sem=self.send.at[self.stages, lax.rem(p, self.signals)],
            recv_sem=self.recv.at[
                self.stages + 1 if middle else self.stages, lax.rem(p, self.signals)
            ],
            device_id={"rep": self.place.inner},
            device_id_type=MESH,
        )

    def outward(self, p):
        return pltpu.make_async_remote_copy(
            src_ref=self.ins(p),
            dst_ref=self.ins(p),
            send_sem=self.send.at[self.stages + 1, lax.rem(p, self.signals)],
            recv_sem=self.recv.at[self.stages + 1, lax.rem(p, self.signals)],
            device_id={"rep": self.place.outer},
            device_id_type=MESH,
        )


def begin(place, lanes, p, mixes):
    advance(place, lanes, jnp.int32(p), p + 1, mixes, only_start=True)


def advance(place, lanes, t, count, mixes, least=0, only_start=False):
    mixes = mixes and place.mixes

    def due(lag, body):
        p = t - lag

        @pl.when(both(p >= 0, p < count))
        def _():
            body(p)

    def each_lane(body):
        for lane in lanes:
            body(lane)

    def mixed(p, body):
        chunk, turn = whole_part(p)
        for fixed in MIXED_TURNS:

            @pl.when(both(turn == fixed, is_mixed(chunk, fixed)))
            def _():
                for lane in lanes:
                    body(lane, p, chunk, fixed, *lane.role(chunk, fixed))

    def together(p, body):
        chunk, turn = whole_part(p)

        @pl.when(turn == SPLIT - 1)
        def _():
            for fixed in MIXED_TURNS:

                @pl.when(is_mixed(chunk, fixed))
                def _():
                    for lane in lanes:
                        at = p + fixed - SPLIT + 1
                        body(lane, at, chunk, fixed, *lane.role(chunk, fixed))

    def early(p, body):
        chunk, turn = whole_part(p)

        @pl.when(turn == 0)
        def _():
            for fixed in MIXED_TURNS:

                @pl.when(is_mixed(chunk, fixed))
                def _():
                    for lane in lanes:
                        body(lane, p + fixed, chunk, fixed)

    def plain(p, body):
        if not mixes:
            each_lane(body)
            return
        chunk, turn = whole_part(p)

        @pl.when(jnp.logical_not(is_mixed(chunk, turn)))
        def _():
            each_lane(body)

    def start(p):
        plain(p, lambda lane: lane.half_copy(0, p).start())
        if mixes:
            early(p, lambda lane, at, chunk, turn: lane.half_copy(0, at).start())

    if only_start:
        start(t)
        return

    @pl.when(both(t >= least, t < count))
    def _():
        start(t)

    def onward(lane, p):
        if place.bits > 1:
            lane.half_copy(1, p).start()

    def first(p):
        def usual(lane):
            lane.arrive(0, p)
            onward(lane, p)

        plain(p, usual)
        if not mixes:
            return

        def taken(lane, p, chunk, turn, gives, takes, misses):
            @pl.when(takes)
            def _():
                lane.raw_copy(p, chunk, turn).wait_recv()
                into = lane.halves(0, p)
                into[...] += lane.raws(lax.rem(chunk, RAW) + (RAW if turn == SPLIT - 2 else 0))[...]

            @pl.when(jnp.logical_not(gives))
            def _():
                onward(lane, p)

        together(p, taken)

        def given(lane, p, chunk, turn):
            lane.arrive(0, p)

            @pl.when(lane.role(chunk, turn)[0])
            def _():
                lane.raw_copy(p, chunk, turn).start()

        early(p, given)

    due(1, first)

    def later(stage):
        def usual(lane, p):
            lane.arrive(stage, p)
            if stage < place.bits - 1:
                lane.half_copy(stage + 1, p).start()
            else:

                @pl.when(place.depth == 0)
                def _():
                    lane.inward(p, place.left == 0).start()

        def body(p):
            plain(p, lambda lane: usual(lane, p))
            if not mixes:
                return

            def special(lane, p, chunk, turn, gives, takes, misses):
                @pl.when(jnp.logical_not(gives))
                def _():
                    usual(lane, p)

                if stage == 1:

                    @pl.when(gives)
                    def _():
                        lane.raw_copy(p, chunk, turn).wait_send()

            mixed(p, special)

        return body

    for stage in range(1, place.bits):
        due(1 + LAG * stage, later(stage))

    def collect(p):
        def go(lane):
            if place.left == 1:
                lane.inward(p, True).start()
            else:
                for middle in (False, True):

                    @pl.when((place.depth == place.left) == middle)
                    def _():
                        lane.inward(p, middle).start()

        def usual(lane):
            lane.inward(p, False).wait_recv()
            into = lane.total(p)
            into[...] += lane.outs(p)[...]
            go(lane)

        def special(lane, p, chunk, turn, gives, takes, misses):
            @pl.when(gives)
            def _():
                lane.inward(p, False).wait_recv()
                lane.total(p)[...] = lane.outs(p)[...]

            @pl.when(jnp.logical_not(jnp.logical_or(gives, misses)))
            def _():
                lane.inward(p, False).wait_recv()
                into = lane.total(p)
                into[...] += lane.outs(p)[...]

            go(lane)

        @pl.when(place.depth > 0)
        def _():
            plain(p, usual)
            if mixes:
                mixed(p, special)

    if place.left > 0:
        due(place.base + HOP * place.depth, collect)

    def share(p):
        for lane in lanes:
            lane.outward(p).wait_recv()

            @pl.when(place.depth == place.left)
            def _(lane=lane):
                into = lane.ins(p)
                into[...] += lane.total(p)[...]

            @pl.when(place.depth > 0)
            def _(lane=lane):
                lane.outward(p).start()

        for lane in lanes:
            lane.finish(p)

    due(place.top + HOP * (place.left - place.depth), share)

    def settle(p):
        def sent(lane):
            lane.inward(p, False).wait_send()

        plain(p, sent)
        if mixes:

            def special(lane, p, chunk, turn, gives, takes, misses):
                @pl.when(jnp.logical_or(place.depth > 0, jnp.logical_not(gives)))
                def _():
                    sent(lane)

            mixed(p, special)

        @pl.when(place.depth > 0)
        def _():
            for lane in lanes:
                lane.outward(p).wait_send()

    due(place.last_step, settle)


def kernel(n_inst, n_rep, *refs):
    order_in, acts, keys_in, values_in, logits_in = refs[:5]
    state_in, state = refs[5:11], refs[11:17]
    order, slabs, keys, values, logits, turned, router_all, parts, router_parts = refs[17:26]
    raws, load = refs[26:28]
    scratch = refs[28:]
    place = Place(n_inst, n_rep)
    bits, rep = place.bits, place.rep
    rows = slabs.shape[-1]
    width = router_parts.shape[-1]
    per_bucket = order.shape[0] // BUCKETS
    column_blocks = acts.shape[1] // BLOCK_ROWS
    chunks = keys.shape[1] // COLS
    every = chunks * BUCKETS // 2
    count = every * SPLIT
    size = COLS // SPLIT
    halves = scratch[:bits]
    router_halves = scratch[bits : 2 * bits]
    outs, ins, router_outs, router_ins = scratch[2 * bits : 2 * bits + 4]
    sends, recvs, router_sends, router_recvs, raw_sends, raw_recvs = scratch[2 * bits + 4 :]

    def finish(kind):
        def body(p):
            chunk, turn = whole_part(p)

            @pl.when(turn == SPLIT - 1)
            def _():
                bucket = 2 * lax.div(chunk, chunks) + kind
                start = pl.multiple_of(lax.rem(chunk, chunks) * COLS, COLS)
                slot = lax.rem(chunk * SPLIT, ins.shape[1])
                grad = ins[kind, pl.ds(slot, SPLIT), 0].reshape(COLS, rows).T
                at = (bucket, slice(None), pl.ds(start, COLS))
                fresh = adamw(grad, *[part[at] for part in state[:3]])
                for part, value in zip(state[:3], fresh):
                    part[at] = value

        return body

    def router_finish(p):
        line = state[3].shape[1]
        for at in range(state[3].shape[0]):
            one = (pl.ds(at, 1), slice(None))
            grad = router_ins[0, :, pl.ds(at * line, line)]
            fresh = adamw(grad, *[part[one] for part in state[3:]])
            for part, value in zip(state[3:], fresh):
                part[one] = value

    forward = [0] + list(range(1, bits))
    backward = [0] + list(range(bits - 1, 0, -1))
    lanes = []
    for kind, dims in enumerate((forward, backward)):
        lanes.append(
            Lane(
                place,
                kind,
                dims,
                (
                    lambda p, kind=kind: parts.at[kind, lax.rem(p, 2 * SPLIT)],
                    lambda stage, p, kind=kind: halves[stage].at[
                        kind, lax.rem(p, halves[stage].shape[1])
                    ],
                    lambda p, kind=kind: outs.at[kind, lax.rem(p, outs.shape[1])],
                    lambda p, kind=kind: ins.at[kind, lax.rem(p, ins.shape[1])],
                    lambda at: raws.at[at],
                ),
                (sends.at[kind], recvs.at[kind], raw_sends, raw_recvs),
                SIGNALS,
                finish(kind),
            )
        )
    router = Lane(
        place,
        0,
        forward,
        (
            lambda p: router_parts,
            lambda stage, p: router_halves[stage],
            lambda p: router_outs,
            lambda p: router_ins,
            None,
        ),
        (router_sends, router_recvs, None, None),
        1,
        router_finish,
    )

    lead, rest = pl.ds(0, COLS), pl.ds(COLS, keys.shape[1] - COLS)
    early = [(order_in, order)]
    early += [(keys_in.at[:, lead], keys.at[:, lead]), (values_in.at[:, lead], values.at[:, lead])]
    early += [
        (acts.at[:, pl.ds(at * rows, rows)], slabs.at[at]) for at in range(slabs.shape[0])
    ]
    late = [(keys_in.at[:, rest], keys.at[:, rest]), (values_in.at[:, rest], values.at[:, rest])]
    late += [(logits_in, logits)]
    late += list(zip(state_in, state))
    loads = [
        pltpu.make_async_copy(src, dst, load.at[at]) for at, (src, dst) in enumerate(early + late)
    ]
    early, late, states = loads[: len(early)], loads[len(early) : -len(state)], loads[-len(state) :]
    for copy in early + late:
        copy.start()

    barrier = pltpu.get_barrier_semaphore()
    for flip in place.flips:
        pl.semaphore_signal(
            barrier, inc=1, device_id={"inst": place.me + flip}, device_id_type=MESH
        )

    @pl.when(rep > 0)
    def _():
        pl.semaphore_signal(barrier, inc=1, device_id={"rep": rep - 1}, device_id_type=MESH)

    @pl.when(rep < n_rep - 1)
    def _():
        pl.semaphore_signal(barrier, inc=1, device_id={"rep": rep + 1}, device_id_type=MESH)

    for copy in early:
        copy.wait()

    each = n_inst // SPLIT

    def turn_over(chunk):
        column = pl.multiple_of(lax.rem(chunk, chunks) * COLS, COLS)
        turned[0] = keys[:, pl.ds(column, COLS)].T
        turned[1] = values[:, pl.ds(column, COLS)].T

    def products(chunk, turn):
        slot = lax.rem(chunk, 2) * SPLIT
        for kind, lane in enumerate(lanes):
            bucket = 2 * lax.div(chunk, chunks) + kind
            for i in range(each):
                q = turn * each + i
                first = lane.owner(q) * rows
                block = order[bucket * per_bucket + lax.div(first, BLOCK_ROWS)]
                at = lax.rem(block, column_blocks) * (BLOCK_ROWS // rows)
                at = at + lax.div(lax.rem(first, BLOCK_ROWS), rows)
                full = jnp.dot(
                    turned[lax.div(block, column_blocks)],
                    slabs[at],
                    preferred_element_type=jnp.float32,
                )
                for part in range(SPLIT):
                    parts[kind, slot + part, q] = full[part * size : (part + 1) * size]

    def router_products():
        for at in range(slabs.shape[0]):
            router_all[:, pl.ds(at * rows, rows)] = jnp.dot(
                logits[...], slabs[at], preferred_element_type=jnp.float32
            )
        for q in range(n_inst):
            first = router.owner(q) * width
            router_parts[q] = router_all[
                pl.ds(first // acts.shape[1], 1),
                pl.ds(pl.multiple_of(first % acts.shape[1], width), width),
            ]

    def head(turn, carry):
        products(0, turn)
        return carry

    turn_over(0)
    lax.fori_loop(SPLIT // 2, SPLIT, head, 0)
    peers = bits + jnp.where(rep > 0, 1, 0) + jnp.where(rep < n_rep - 1, 1, 0)
    pl.semaphore_wait(barrier, peers)
    begin(place, lanes, 0, True)
    lax.fori_loop(0, SPLIT // 2, head, 0)
    for copy in states:
        copy.start()
    for copy in late:
        copy.wait()

    def step(t, carry):
        advance(place, lanes, t, count, True, least=1)

        @pl.when(t == ROUTER_START)
        def _():
            router_products()
            for copy in states:
                copy.wait()

        @pl.when(both(t >= ROUTER_START, t <= ROUTER_START + place.last_step))
        def _():
            advance(place, [router], t - ROUTER_START, 1, False)

        @pl.when(t < count - SPLIT)
        def _():
            chunk, turn = lax.div(t, SPLIT) + 1, lax.rem(t, SPLIT)

            @pl.when(turn == 0)
            def _():
                turn_over(chunk)

            products(chunk, turn)

        return carry

    lax.fori_loop(0, count + place.last_step, step, 0)


def summed(order, acts, keys, values, logits, states, n_inst, n_rep):
    bits = n_inst.bit_length() - 1
    rows = states[0].shape[1]
    width = states[3].size
    kv = keys.shape[1]
    size = COLS // SPLIT
    every = kv // COLS * BUCKETS // 2
    count = every * SPLIT
    vmem = pl.BlockSpec(memory_space=pltpu.VMEM)
    f32 = jnp.float32
    scratch = [
        pltpu.SMEM(order.shape, order.dtype),
        pltpu.VMEM((acts.shape[1] // rows, acts.shape[0], rows), acts.dtype),
        pltpu.VMEM(keys.shape, keys.dtype),
        pltpu.VMEM(values.shape, values.dtype),
        pltpu.VMEM(logits.shape, logits.dtype),
        pltpu.VMEM((2, COLS, acts.shape[0]), acts.dtype),
        pltpu.VMEM((logits.shape[0], acts.shape[1]), f32),
        pltpu.VMEM((2, 2 * SPLIT, n_inst, size, rows), f32),
        pltpu.VMEM((n_inst, 1, width), f32),
        pltpu.VMEM((2 * RAW, n_inst // 2, size, rows), f32),
        pltpu.SemaphoreType.DMA((acts.shape[1] // rows + 6 + len(states),)),
    ]
    scratch += [
        pltpu.VMEM((2, min(count, FAR if s else NEAR), n_inst >> (s + 1), size, rows), f32)
        for s in range(bits)
    ]
    scratch += [pltpu.VMEM((n_inst >> (s + 1), 1, width), f32) for s in range(bits)]
    scratch += [pltpu.VMEM((2, min(count, FAR), 1, size, rows), f32)] * 2
    scratch += [pltpu.VMEM((1, 1, width), f32)] * 2
    scratch += [pltpu.SemaphoreType.DMA((2, bits + 2, SIGNALS))] * 2
    scratch += [pltpu.SemaphoreType.DMA((bits + 2, 1))] * 2
    scratch += [pltpu.SemaphoreType.DMA((2 * RAW,))] * 2
    operands = (order, acts, keys, values, logits, *states)
    return pl.pallas_call(
        functools.partial(kernel, n_inst, n_rep),
        out_shape=tuple(jax.ShapeDtypeStruct(s.shape, s.dtype) for s in states),
        in_specs=[pl.BlockSpec(memory_space=pltpu.HBM)] * len(operands),
        out_specs=(vmem,) * len(states),
        scratch_shapes=scratch,
        compiler_params=pltpu.CompilerParams(
            collective_id=0, has_side_effects=True, vmem_limit_bytes=VMEM_BYTES
        ),
        cost_estimate=pl.CostEstimate(
            flops=4 * acts.shape[0] * acts.shape[1] * kv,
            bytes_accessed=24 * 2**20,
            transcendentals=0,
        ),
    )(*[pltpu.with_memory_space_constraint(x, pltpu.HBM) for x in operands])


def write_kernel(*refs):
    many = (len(refs) - 1) // 2
    copies = [
        pltpu.make_async_copy(refs[at], refs[many + at], refs[-1].at[at]) for at in range(many)
    ]
    for copy in copies:
        copy.start()
    for copy in copies:
        copy.wait()


def written(arrays):
    return pl.pallas_call(
        write_kernel,
        out_shape=tuple(jax.ShapeDtypeStruct(a.shape, a.dtype) for a in arrays),
        in_specs=[pl.BlockSpec(memory_space=pl.ANY)] * len(arrays),
        out_specs=(pl.BlockSpec(memory_space=pltpu.HBM),) * len(arrays),
        scratch_shapes=[pltpu.SemaphoreType.DMA((len(arrays),))],
        compiler_params=pltpu.CompilerParams(vmem_limit_bytes=2**20),
        cost_estimate=pl.CostEstimate(flops=2**20, bytes_accessed=24 * 2**20, transcendentals=0),
    )(*arrays)


def on_device(n_inst, n_rep, acts, grad_keys, grad_values, grad_logits, order, *states):
    fresh = summed(order, acts, grad_keys, grad_values, grad_logits, states, n_inst, n_rep)
    return written(fresh)


def solution(mesh):
    return jax.shard_map(
        functools.partial(on_device, mesh.shape["inst"], mesh.shape["rep"]),
        mesh=mesh,
        in_specs=(
            P(("rep", "inst"), None),
            P(("rep", "inst"), None),
            P(("rep", "inst"), None),
            P(None, ("rep", "inst")),
            P(),
            P(None, "inst", None),
            P(None, "inst", None),
            P(None, "inst", None),
            P("inst", None),
            P("inst", None),
            P("inst", None),
        ),
        out_specs=(
            P(None, "inst", None),
            P(None, "inst", None),
            P(None, "inst", None),
            P("inst", None),
            P("inst", None),
            P("inst", None),
        ),
        check_vma=False,
    )
```
